512 devices in a mesh: slab: 64 (over z, y_hi, core), load: 8 (over x, y_lo).
Axes of the slice: x: 4, y: 8 (y_hi: 4, y_lo: 2; y = y_hi * 2 + y_lo), z: 8, core: 2. Of those that a mesh axis runs over, the one named last changes fastest.
Arguments:
- density: float32 [256, 16, 128], P('slab'), may hold values from 0.05 to 1
- passive: int32 [256, 16, 128], P('slab'), may hold values 0 or 1
- fixed: int32 [256, 16, 128], P('slab'), may hold values 0 or 1
- u_start: float32 [8, 3, 256, 16, 128], P('load', None, 'slab'), may hold values from -4 to 4
- load_nodes: int32 [8, 64], P('load'), may hold values from 0 to 524287
- load_forces: float32 [8, 3, 64], P('load'), may hold values from -6 to 6
Outputs:
- new_density: float32 [256, 16, 128], P('slab', 'load')
- displacement: float32 [8, 3, 256, 16, 128], P('load', None, 'slab')
The draws below stay inside these ranges and needn't reach their ends.
All inputs are finite; a program needn't handle non-finite values. No bound on the sum of `passive` or of `fixed` on one device may be relied on, other than what follows from the above.
Results may differ from the reference program's by a relative error of at most 0.0003.
Values sent between devices are 32-bit elements; how exact they have to be, the bound alone decides.
A program may use at most 64 MiB of HBM per device.

```python
import math
import jax
import jax.numpy as jnp
import numpy as np
from jax import lax

NX = 128
NY = 16
NPTS = 64
SWEEPS = 3
UPDATES = 2
NZ = 256
LOADS = 8


def draw_density(key, part):
    second = jax.random.fold_in(jax.random.fold_in(key, 11), 1)
    height = (jnp.arange(NZ, dtype=jnp.float32) + 0.5) / NZ
    base = 0.25 + 0.5 * height
    rough = jax.random.uniform(second, (NZ, NY, NX), jnp.float32, 0.6, 1.3)
    return jnp.clip(base[:, None, None] * rough, 0.05, 1.0)


def touch_ends(values, own_key, smallest, high):
    spot = [jax.random.randint(jax.random.fold_in(own_key, axis), (), 0, length) for axis, length in enumerate(values.shape)]
    widest = values.shape.index(max(values.shape))
    beside = spot[:widest] + [(spot[widest] + 1) % values.shape[widest]] + spot[widest + 1:]
    return values.at[tuple(spot)].set(smallest).at[tuple(beside)].set(high)


def steps_of(own_key, dims, cuts, low, largest):
    factor_of, own = 1.0, jax.random.fold_in(own_key, 6)
    for dim, shards_of in cuts:
        heights = jnp.exp(jax.random.uniform(jax.random.fold_in(own, dim), (shards_of,), jnp.float32, low / len(cuts), largest / len(cuts)))
        factor_of = factor_of * jnp.repeat(heights, dims[dim] // shards_of).reshape([-1 if axis == dim else 1 for axis in range(len(dims))])
    return factor_of


def noise(key, shape, deviation, limit, cuts=(), kind=jnp.bfloat16):
    values = jax.random.normal(key, shape, jnp.float32) * deviation
    if len(cuts) > 0:
        values = steps_of(key, shape, cuts, -0.22, 0.18) * values
    return jnp.clip(values, min=-limit, max=limit).astype(kind)


def setup_inputs(seed: int = 0) -> dict:
    keys = jax.random.split(jax.random.key(seed), 7)
    density = draw_density(jax.random.fold_in(keys[6], 71), 0)
    passive = touch_ends((jax.random.randint(keys[1], (NZ, NY, NX), 0, 8) < 1).astype(jnp.int32), jax.random.fold_in(keys[1], 1), 0, 1)
    fixed = touch_ends((jax.random.randint(keys[2], (NZ, NY, NX), 0, 16) < 1).astype(jnp.int32), jax.random.fold_in(keys[2], 1), 0, 1)
    u_start = noise(keys[3], (LOADS, 3, NZ, NY, NX), 0.5, 4.0, ((0, 8), (2, 64)), jnp.float32)
    load_nodes = touch_ends(jax.random.randint(keys[4], (LOADS, NPTS), 0, NZ * NY * NX), jax.random.fold_in(keys[4], 1), 0, (NZ * NY * NX) - 1).astype(jnp.int32)
    load_forces = noise(keys[5], (LOADS, 3, NPTS), 1.0, 6.0, ((0, 8),), jnp.float32)
    return dict(density=density, passive=passive, fixed=fixed, u_start=u_start, load_nodes=load_nodes, load_forces=load_forces)


young_floor = 0.001
density_floor = 0.001
move_limit = 0.2
sens_shift = 0.001

def diagonal_of(matrix):
    return np.array([matrix[entry, entry] for entry in range(matrix.shape[0])])

def element_stiffness():
    poisson = 0.3
    lame_first = poisson / ((1.0 + poisson) * (1.0 - 2.0 * poisson))
    lame_second = 1.0 / (2.0 * (1.0 + poisson))
    elastic = np.zeros((6, 6))
    elastic[:3, :3] = lame_first
    for axis_pos in range(3):
        elastic[axis_pos, axis_pos] += 2.0 * lame_second
        elastic[axis_pos + 3, axis_pos + 3] = lame_second
    points = [0.5 - 0.5 / math.sqrt(3.0), 0.5 + 0.5 / math.sqrt(3.0)]
    matrix = np.zeros((24, 24))
    for point_x in points:
        for point_y in points:
            for point_z in points:
                strain = np.zeros((6, 24))
                for corner in range(8):
                    shift_x = corner % 2
                    shift_y = corner // 2 % 2
                    shift_z = corner // 4
                    value_x = point_x if shift_x else 1.0 - point_x
                    value_y = point_y if shift_y else 1.0 - point_y
                    value_z = point_z if shift_z else 1.0 - point_z
                    slope_x = 1.0 if shift_x else -1.0
                    slope_y = 1.0 if shift_y else -1.0
                    slope_z = 1.0 if shift_z else -1.0
                    grad_x = slope_x * value_y * value_z
                    grad_y = value_x * slope_y * value_z
                    grad_z = value_x * value_y * slope_z
                    column = 3 * corner
                    strain[0, column] = grad_x
                    strain[1, column + 1] = grad_y
                    strain[2, column + 2] = grad_z
                    strain[3, column] = grad_y
                    strain[3, column + 1] = grad_x
                    strain[4, column + 1] = grad_z
                    strain[4, column + 2] = grad_y
                    strain[5, column] = grad_z
                    strain[5, column + 2] = grad_x
                matrix += strain.T @ elastic @ strain / 8.0
    return matrix

def spectrum_top(matrix):
    diag_np = diagonal_of(matrix)
    scaled = matrix / np.sqrt(np.outer(diag_np, diag_np))
    vector = np.linspace(1.0, 2.0, 24)
    for repeat in range(500):
        vector = scaled @ vector
        vector = vector / np.sqrt(np.sum(vector * vector))
    return float(vector @ scaled @ vector)

def cheb_constants(matrix):
    upper_bound = 1.05 * spectrum_top(matrix)
    lower_bound = upper_bound / 12.0
    center = 0.5 * (upper_bound + lower_bound)
    half_width = 0.5 * (upper_bound - lower_bound)
    return (center, half_width, center / half_width)

def cheb_weights(count, half_width, ratio_sigma):
    weights = []
    current = 1.0 / ratio_sigma
    for iteration in range(count):
        following = 1.0 / (2.0 * ratio_sigma - current)
        weights.append((following * current, 2.0 * following / half_width))
        current = following
    return weights

def element_values(field):
    planes = field.shape[2] - 1
    rows = field.shape[3]
    cols = field.shape[4]
    padded = jnp.pad(field, ((0, 0), (0, 0), (0, 0), (0, 1), (0, 1)))
    pieces = []
    for corner in range(8):
        shift_x = corner % 2
        shift_y = corner // 2 % 2
        shift_z = corner // 4
        pieces.append(padded[:, :, shift_z:shift_z + planes, shift_y:shift_y + rows, shift_x:shift_x + cols])
    stacked = jnp.stack(pieces, axis=1)
    return stacked.reshape(field.shape[0], 24, planes, rows, cols)

def spread_nodes(forces):
    cases, planes, rows, cols = (forces.shape[0], forces.shape[2], forces.shape[3], forces.shape[4])
    split = forces.reshape(cases, 8, 3, planes, rows, cols)
    total = jnp.zeros((cases, 3, planes + 1, rows + 1, cols + 1), jnp.float32)
    for corner in range(8):
        shift_x = corner % 2
        shift_y = corner // 2 % 2
        shift_z = corner // 4
        total = total + jnp.pad(split[:, corner], ((0, 0), (0, 0), (shift_z, 1 - shift_z), (shift_y, 1 - shift_y), (shift_x, 1 - shift_x)))
    return total[:, :, :, :rows, :cols]

def stiff_apply(values, table):
    return jnp.einsum('ij,cjzyx->cizyx', table, values, precision=lax.Precision.HIGHEST)

def top_padded(field):
    return jnp.pad(field, ((0, 0), (0, 0), (0, 1), (0, 0), (0, 0)))

def operate(field, young, table):
    values = element_values(top_padded(field))
    spread = spread_nodes(young[None, None] * stiff_apply(values, table))
    return spread[:, :, :field.shape[2]]

def reference(density, passive, fixed, u_start, load_nodes, load_forces):
    stiff_numpy = element_stiffness()
    center, half_width, ratio_sigma = cheb_constants(stiff_numpy)
    table = jnp.asarray(stiff_numpy, jnp.float32)
    planes, rows, cols = density.shape
    count = planes * rows * cols
    free = (1 - fixed).astype(jnp.float32)
    void = passive == 1
    active = (1 - passive).astype(jnp.float32)
    design = jnp.where(void, jnp.float32(density_floor), density)

    def place(nodes, values):
        return jnp.zeros((3, count), jnp.float32).at[:, nodes.astype(jnp.int32)].add(values)
    loads = jax.vmap(place)(load_nodes, load_forces).reshape(load_nodes.shape[0], 3, planes, rows, cols)
    diag_table = jnp.asarray(diagonal_of(stiff_numpy), jnp.float32)
    weights = cheb_weights(SWEEPS, half_width, ratio_sigma)
    displace = u_start
    for update in range(UPDATES):
        young = young_floor + (1.0 - young_floor) * design * design * design
        diag_terms = young[None, None] * diag_table[None, :, None, None, None]
        diagonal = spread_nodes(diag_terms)[:, :, :planes]
        inverse = free / diagonal
        displace = displace * free
        residual = free * (loads - operate(displace, young, table))
        direction = inverse * residual / center
        for iteration in range(SWEEPS):
            displace = displace + direction
            if iteration < SWEEPS - 1:
                residual = residual - free * operate(direction, young, table)
                keep, push = weights[iteration]
                direction = keep * direction + push * inverse * residual
        values = element_values(top_padded(displace))
        energy = lax.optimization_barrier(jnp.sum(values * stiff_apply(values, table), axis=1))
        total = lax.optimization_barrier(jnp.sum(energy, axis=0))
        quantity = design * jnp.sqrt(3.0 * design * design * (1.0 - young_floor) * total + sens_shift)
        scale = jnp.sum(quantity * active) / jnp.sum(design * active)
        lower = jnp.maximum(density_floor, design - move_limit)
        upper = jnp.minimum(1.0, design + move_limit)
        design = jnp.where(void, jnp.float32(density_floor), jnp.clip(quantity / scale, lower, upper))
    return (design, displace)
```

```python
import functools
import math

import jax
import jax.numpy as jnp
import numpy as np
from jax import lax
from jax.experimental import pallas as pl
from jax.experimental.pallas import tpu as pltpu
from jax.sharding import PartitionSpec as P

SWEEPS = 3
UPDATES = 2
MESH = pl.DeviceIdType.MESH
young_floor = 0.001
density_floor = 0.001
move_limit = 0.2
sens_shift = 0.001
BELOW = 3
ABOVE = 4


def diagonal_of(matrix):
    return np.array([matrix[entry, entry] for entry in range(matrix.shape[0])])


def element_stiffness():
    poisson = 0.3
    lame_first = poisson / ((1.0 + poisson) * (1.0 - 2.0 * poisson))
    lame_second = 1.0 / (2.0 * (1.0 + poisson))
    elastic = np.zeros((6, 6))
    elastic[:3, :3] = lame_first
    for axis_pos in range(3):
        elastic[axis_pos, axis_pos] += 2.0 * lame_second
        elastic[axis_pos + 3, axis_pos + 3] = lame_second
    points = [0.5 - 0.5 / math.sqrt(3.0), 0.5 + 0.5 / math.sqrt(3.0)]
    matrix = np.zeros((24, 24))
    for point_x in points:
        for point_y in points:
            for point_z in points:
                strain = np.zeros((6, 24))
                for corner in range(8):
                    shift_x = corner % 2
                    shift_y = corner // 2 % 2
                    shift_z = corner // 4
                    value_x = point_x if shift_x else 1.0 - point_x
                    value_y = point_y if shift_y else 1.0 - point_y
                    value_z = point_z if shift_z else 1.0 - point_z
                    slope_x = 1.0 if shift_x else -1.0
                    slope_y = 1.0 if shift_y else -1.0
                    slope_z = 1.0 if shift_z else -1.0
                    grad_x = slope_x * value_y * value_z
                    grad_y = value_x * slope_y * value_z
                    grad_z = value_x * value_y * slope_z
                    column = 3 * corner
                    strain[0, column] = grad_x
                    strain[1, column + 1] = grad_y
                    strain[2, column + 2] = grad_z
                    strain[3, column] = grad_y
                    strain[3, column + 1] = grad_x
                    strain[4, column + 1] = grad_z
                    strain[4, column + 2] = grad_y
                    strain[5, column] = grad_z
                    strain[5, column + 2] = grad_x
                matrix += strain.T @ elastic @ strain / 8.0
    return matrix


def spectrum_top(matrix):
    diag_np = diagonal_of(matrix)
    scaled = matrix / np.sqrt(np.outer(diag_np, diag_np))
    vector = np.linspace(1.0, 2.0, 24)
    for repeat in range(500):
        vector = scaled @ vector
        vector = vector / np.sqrt(np.sum(vector * vector))
    return float(vector @ scaled @ vector)


def cheb_constants(matrix):
    upper_bound = 1.05 * spectrum_top(matrix)
    lower_bound = upper_bound / 12.0
    center = 0.5 * (upper_bound + lower_bound)
    half_width = 0.5 * (upper_bound - lower_bound)
    return (center, half_width, center / half_width)


def cheb_weights(count, half_width, ratio_sigma):
    weights = []
    current = 1.0 / ratio_sigma
    for iteration in range(count):
        following = 1.0 / (2.0 * ratio_sigma - current)
        weights.append((following * current, 2.0 * following / half_width))
        current = following
    return weights


def parity_stiffness(matrix):
    transform = np.zeros((24, 24))
    for mode in range(8):
        for corner in range(8):
            sign = 1.0
            for axis in range(3):
                if (mode >> axis) & 1 and not (corner >> axis) & 1:
                    sign = -sign
            for part in range(3):
                transform[3 * mode + part, 3 * corner + part] = sign
    return transform @ matrix @ transform.T / 64.0


def mode_constants(matrix):
    block = parity_stiffness(matrix)

    def entry(part_a, mode_a, part_b, mode_b):
        def index(part, mode):
            return 3 * sum(1 << axis for axis in range(3) if mode[axis] == "d") + part

        return float(block[index(part_a, mode_a), index(part_b, mode_b)])

    cross = entry(0, "dss", 1, "sds")
    return dict(
        cross=cross,
        normal=entry(0, "dss", 0, "dss") - cross,
        shear=entry(0, "sds", 1, "dss"),
        bend=entry(0, "dds", 0, "dds"),
        couple=entry(0, "dds", 2, "sdd"),
        twist=entry(0, "sdd", 1, "dsd"),
        warp=entry(0, "ddd", 0, "ddd"),
    )


def right_of(value, lane):
    return jnp.where(lane == value.shape[1] - 1, 0.0, pltpu.roll(value, value.shape[1] - 1, 1))


def left_of(value, lane):
    return jnp.where(lane == 0, 0.0, pltpu.roll(value, 1, 1))


def under_of(value, row):
    return jnp.where(row == 0, 0.0, pltpu.roll(value, 1, 0))


def plane_modes(ref, plane, lane, rows):
    found = []
    for part in range(3):
        near = ref[part, plane, 0:rows, :]
        far = ref[part, plane, 1 : rows + 1, :]
        for value in (near + far, far - near):
            other = right_of(value, lane)
            found += [value + other, other - value]
    return found


def element_modes(low, high):
    names = ("ss", "ds", "sd", "dd")
    modes = {}
    for part in range(3):
        for place, name in enumerate(names):
            low_value, high_value = low[4 * part + place], high[4 * part + place]
            if name != "ss":
                modes["xyz"[part] + name + "s"] = low_value + high_value
            modes["xyz"[part] + name + "d"] = high_value - low_value
    return modes


def stress_modes(m, young, k):
    normal, cross, shear = young * k["normal"], young * k["cross"], young * k["shear"]
    bend, couple, twist = young * k["bend"], young * k["couple"], young * k["twist"]
    warp = young * k["warp"]
    out = {}
    trace = cross * (m["xdss"] + m["ysds"] + m["zssd"])
    for name in ("xdss", "ysds", "zssd"):
        out[name] = normal * m[name] + trace
    for first, second in (("ydss", "xsds"), ("zdss", "xssd"), ("zsds", "yssd")):
        out[first] = out[second] = shear * (m[first] + m[second])
    for first, second in (("xdds", "zsdd"), ("ydds", "zdsd"), ("xdsd", "ysdd")):
        out[first] = bend * m[first] + couple * m[second]
        out[second] = couple * m[first] + bend * m[second]
    total = m["zdds"] + m["ydsd"] + m["xsdd"]
    for name in ("zdds", "ydsd", "xsdd"):
        out[name] = twist * (m[name] + total)
    for name in ("xddd", "yddd", "zddd"):
        out[name] = warp * m[name]
    return out


def energy_of(m, k):
    def squares(names):
        return sum((m[name] * m[name] for name in names[1:]), m[names[0]] * m[names[0]])

    normals = ("xdss", "ysds", "zssd")
    twists = ("zdds", "ydsd", "xsdd")
    trace = m["xdss"] + m["ysds"] + m["zssd"]
    result = k["normal"] * squares(normals) + k["cross"] * (trace * trace)
    shears = None
    for first, second in (("ydss", "xsds"), ("zdss", "xssd"), ("zsds", "yssd")):
        value = m[first] + m[second]
        shears = value * value if shears is None else shears + value * value
    result = result + k["shear"] * shears
    pairs = (("xdds", "zsdd"), ("ydds", "zdsd"), ("xdsd", "ysdd"))
    result = result + k["bend"] * squares([name for pair in pairs for name in pair])
    products = sum(
        (m[first] * m[second] for first, second in pairs[1:]), m[pairs[0][0]] * m[pairs[0][1]]
    )
    result = result + (2.0 * k["couple"]) * products
    total = m["zdds"] + m["ydsd"] + m["xsdd"]
    result = result + k["twist"] * (squares(twists) + total * total)
    return result + k["warp"] * squares(("xddd", "yddd", "zddd"))


def node_parts(out):
    lower, upper = [], []
    for part in "xyz":
        for name in ("ss", "ds", "sd", "dd"):
            odd = out[part + name + "d"]
            if name == "ss":
                lower.append(-odd)
                upper.append(odd)
            else:
                even = out[part + name + "s"]
                lower.append(even - odd)
                upper.append(even + odd)
    return lower, upper


def node_force(sums, lane, row):
    forces = []
    for part in range(3):
        both, along, across, twice = sums[4 * part : 4 * part + 4]
        even = (both - along) + left_of(both + along, lane)
        odd = (across - twice) + left_of(across + twice, lane)
        forces.append((even - odd) + under_of(even + odd, row))
    return forces


def apply_stiffness(ref, first, count, young_ref, young_first, k, lane, row, emit):
    rows = row.shape[0]
    low = plane_modes(ref, first - 1, lane, rows)
    high = plane_modes(ref, first, lane, rows)
    out = stress_modes(element_modes(low, high), young_ref[young_first - 1], k)
    pending = node_parts(out)[1]

    def step(turn, carry):
        low, pending = carry
        high = plane_modes(ref, first + 1 + turn, lane, rows)
        out = stress_modes(element_modes(low, high), young_ref[young_first + turn], k)
        lower, upper = node_parts(out)
        emit(turn, node_force([a + b for a, b in zip(lower, pending)], lane, row))
        return high, upper

    lax.fori_loop(0, count, step, (high, pending), unroll=True)


def kernel(
    k, chebyshev, stiff_diag, slabs, loads,
    density_hbm, passive_hbm, fixed_hbm, start_hbm, nodes_ref, points_ref,
    density_out, displace_out,
    fixed_buf, design_buf, passive_buf, raw_buf, masked_buf, first_dir, second_dir, final_buf,
    residual, young_buf, weight_buf, force_buf, share_design, share_active, share_energy,
    gathered_energy, gathered_q, q_buf, stage_a, stage_b, local_sem, halo_send, halo_recv,
    q_halo_send, q_halo_recv, group_send, group_recv,
):
    center, weights = chebyshev
    slab = lax.axis_index("slab")
    load = lax.axis_index("load")
    planes, rows, cols = passive_buf.shape
    own = slice(BELOW, BELOW + planes)
    lane = lax.broadcasted_iota(jnp.int32, (rows, cols), 1)
    row = lax.broadcasted_iota(jnp.int32, (rows, cols), 0)
    up = lax.rem(slab + 1, slabs)
    down = lax.rem(slab + slabs - 1, slabs)
    column = lax.div(slab, 8)
    seat = lax.rem(slab, 8)
    x_place = lax.div(load, 2)
    y_low = lax.rem(load, 2)
    me_a = seat * 2 + y_low
    me_b = column * 4 + x_place

    def member_load(step):
        other = lax.rem(load + step, loads)
        return other, (slab, other)

    def member_a(step):
        other = lax.rem(me_a + step, 16)
        return other, (column * 8 + lax.div(other, 2), x_place * 2 + lax.rem(other, 2))

    def member_b(step):
        other = lax.rem(me_b + step, 32)
        return other, (lax.div(other, 4) * 8 + seat, lax.rem(other, 4) * 2 + y_low)

    groups = ((member_load, 8), (member_a, 16), (member_b, 32))

    copies = [
        pltpu.make_async_copy(start_hbm, raw_buf.at[0, :, own], local_sem.at[0]),
        pltpu.make_async_copy(fixed_hbm, fixed_buf.at[own], local_sem.at[1]),
        pltpu.make_async_copy(density_hbm, design_buf.at[0, own], local_sem.at[2]),
        pltpu.make_async_copy(passive_hbm, passive_buf, local_sem.at[3]),
    ]
    for copy in copies:
        copy.start()

    barrier = pltpu.get_barrier_semaphore()
    for target in ((up, load), (down, load)):
        pl.semaphore_signal(barrier, inc=1, device_id=target, device_id_type=MESH)
    for member, size in groups:

        def greet(step, carry):
            pl.semaphore_signal(barrier, inc=1, device_id=member(step)[1], device_id_type=MESH)
            return carry

        lax.fori_loop(1, size, greet, 0, unroll=True)

    for copy in copies:
        copy.wait()
    for plane in range(planes):
        void = passive_buf[plane] == 1
        value = jnp.where(void, density_floor, design_buf[0, BELOW + plane])
        design_buf[0, BELOW + plane] = value
        active = 1.0 - passive_buf[plane].astype(jnp.float32)
        for part in range(loads):
            share_design[part, 2 * plane : 2 * plane + 2] = value[2 * part : 2 * part + 2]
            share_active[part, 2 * plane : 2 * plane + 2] = active[2 * part : 2 * part + 2]
    pl.semaphore_wait(barrier, 2 + sum(size - 1 for member, size in groups))

    def halo(buf, lead, upward, downward, index, send, recv):
        top = BELOW + planes
        pairs = (
            (slice(top - upward, top), slice(BELOW - upward, BELOW), up),
            (slice(BELOW, BELOW + downward), slice(top, top + downward), down),
        )
        made = []
        for place, (source, target, who) in enumerate(pairs):
            made.append(
                pltpu.make_async_remote_copy(
                    buf.at[lead + (source,)],
                    buf.at[lead + (target,)],
                    send.at[2 * index + place],
                    recv.at[2 * index + place],
                    device_id=(who, load),
                    device_id_type=MESH,
                )
            )
        for copy in made:
            copy.start()
        return made

    def send_group(group, index, source, target_of):
        member, size = groups[group]

        def go(step, carry):
            other, who = member(step)
            source_ref, target_ref = source(other), target_of
            pltpu.make_async_remote_copy(
                source_ref,
                target_ref,
                group_send.at[index],
                group_recv.at[index],
                device_id=who,
                device_id_type=MESH,
            ).start()
            return carry

        lax.fori_loop(1, size, go, 0, unroll=True)

    def await_group(sem, index, ref):
        pltpu.make_async_copy(ref, ref, sem.at[index]).wait()

    u_halos = [halo(raw_buf, (0, slice(None)), BELOW, ABOVE, 0, halo_send, halo_recv)]
    f_halo = halo(fixed_buf, (), BELOW, ABOVE, 1, halo_send, halo_recv)
    x_halo = halo(design_buf, (0,), BELOW, BELOW, 2, halo_send, halo_recv)

    edge = jnp.zeros((8, cols), jnp.float32)
    for part in range(3):
        for buf in (first_dir, second_dir, final_buf):
            for plane in range(buf.shape[1]):
                buf[part, plane, rows : rows + 8] = edge
        for plane in range(masked_buf.shape[2]):
            masked_buf[0, part, plane, rows : rows + 8] = edge
            masked_buf[1, part, plane, rows : rows + 8] = edge

    nodes = nodes_ref[...]
    points = nodes.shape[1]
    tall = 9 * rows
    place_zy = lax.broadcasted_iota(jnp.int32, (tall, points), 0) + (slab * planes - 2) * rows
    hit_zy = jnp.where(lax.div(nodes, cols) == place_zy, 1.0, 0.0)
    hit_x = lax.rem(nodes, cols) == lax.broadcasted_iota(jnp.int32, (cols, points), 0)
    for part in range(3):
        amount = jnp.where(hit_x, points_ref[0, part : part + 1, :], 0.0)
        force_buf[part] = lax.dot_general(
            hit_zy,
            amount,
            (((1,), (1,)), ((), ())),
            precision=lax.Precision.HIGHEST,
            preferred_element_type=jnp.float32,
        ).reshape(9, rows, cols)

    has_below = jnp.where(slab > 0, 1.0, 0.0)
    has_above = jnp.where(slab < slabs - 1, 1.0, 0.0)

    def young_planes(which):
        for plane in range(10):
            x = design_buf[which, plane]
            young = young_floor + (1.0 - young_floor) * x * x * x
            if plane < BELOW:
                young = young * has_below
            elif plane >= BELOW + planes:
                young = young * has_above
            young_buf[which, plane] = young

    for copies_in in (u_halos[0], f_halo, x_halo):
        for copy in copies_in:
            copy.wait_recv()

    def inverse_scale(update):
        await_group(group_recv, 4 * update + 2, stage_b.at[update, 0:31, 0:2])
        sums = jnp.sum(jnp.sum(stage_b[update, :, 0:2], axis=0), axis=1, keepdims=True)
        top, bottom = sums[0:1], sums[1:2]
        ratio = bottom / jnp.where(top > 0.0, top, 1.0)
        return jnp.where(top > 0.0, ratio, 0.0)

    for update in range(UPDATES):
        last = update == UPDATES - 1
        for plane in range(11):
            free = 1.0 - fixed_buf[plane].astype(jnp.float32)
            if plane < BELOW:
                free = free * has_below
            elif plane >= BELOW + planes:
                free = free * has_above
            for part in range(3):
                masked_buf[update, part, plane, 0:rows] = free * raw_buf[update, part, plane]
        if update:
            scale = inverse_scale(0)
            for plane in range(10):
                x = design_buf[0, plane]
                lower = jnp.maximum(density_floor, x - move_limit)
                upper = jnp.minimum(1.0, x + move_limit)
                design_buf[1, plane] = jnp.minimum(
                    jnp.maximum(q_buf[plane] * scale, lower), upper
                )
        young_planes(update)
        for node in range(9):
            free = 1.0 - fixed_buf[node + 1].astype(jnp.float32)
            if node < 2:
                free = free * has_below
            elif node >= 2 + planes:
                free = free * has_above
            around = young_buf[update, node] + young_buf[update, node + 1]
            around = around + under_of(around, row)
            around = around + left_of(around, lane)
            weight_buf[node] = free / jnp.maximum(stiff_diag * around, 1e-6)

        field = masked_buf.at[update]
        young = young_buf.at[update]

        def start_stage(turn, forces):
            weight = weight_buf[turn]
            for part in range(3):
                left = force_buf[part, turn] - forces[part]
                residual[part, turn] = left
                first_dir[part, turn, 0:rows] = (weight * left) / center

        apply_stiffness(field, 1, 9, young, 1, k, lane, row, start_stage)

        def middle_stage(turn, forces):
            weight = weight_buf[turn + 1]
            keep, push = weights[0]
            for part in range(3):
                left = residual[part, turn + 1] - forces[part]
                residual[part, turn + 1] = left
                second_dir[part, turn, 0:rows] = (
                    keep * first_dir[part, turn + 1, 0:rows] + push * weight * left
                )

        apply_stiffness(first_dir, 1, 7, young, 2, k, lane, row, middle_stage)

        def final_stage(turn, forces):
            weight = weight_buf[turn + 2]
            keep, push = weights[1]
            for part in range(3):
                left = residual[part, turn + 2] - forces[part]
                second = second_dir[part, turn + 1, 0:rows]
                final_buf[part, turn, 0:rows] = (
                    field[part, turn + BELOW, 0:rows]
                    + first_dir[part, turn + 2, 0:rows]
                    + second
                    + (keep * second + push * weight * left)
                )

        apply_stiffness(second_dir, 1, 5, young, 3, k, lane, row, final_stage)

        if not last:
            for part in range(3):
                raw_buf[1, part, own] = final_buf[part, 0:planes, 0:rows]
            u_halos.append(halo(raw_buf, (1, slice(None)), BELOW, ABOVE, 3, halo_send, halo_recv))
        else:
            writes = pltpu.make_async_copy(
                final_buf.at[:, 0:planes, 0:rows], displace_out, local_sem.at[0]
            )
            writes.start()

        low = plane_modes(final_buf, 0, lane, rows)
        for plane in range(planes):
            high = plane_modes(final_buf, plane + 1, lane, rows)
            energy = energy_of(element_modes(low, high), k)
            for part in range(loads):
                share_energy[update, part, 2 * plane : 2 * plane + 2] = energy[
                    2 * part : 2 * part + 2
                ]
            low = high
        gathered_energy[update, load] = share_energy[update, load]
        send_group(
            0, 4 * update, lambda other: share_energy.at[update, other], gathered_energy.at[update, load]
        )

        if update == 0:
            x_share = share_design[load]
        else:
            lower = jnp.maximum(density_floor, x_share - move_limit)
            upper = jnp.minimum(1.0, x_share + move_limit)
            x_share = jnp.minimum(jnp.maximum(q_share * scale, lower), upper)
        active = share_active[load]
        await_group(group_recv, 4 * update, gathered_energy.at[update, 0 : loads - 1])
        total = gathered_energy[update, 0]
        for part in range(1, loads):
            total = total + gathered_energy[update, part]
        q_share = (
            x_share
            * jnp.sqrt(3.0 * x_share * x_share * (1.0 - young_floor) * total + sens_shift)
            * active
        )
        sums = jnp.concatenate(
            [
                jnp.sum(q_share, axis=0, keepdims=True),
                jnp.sum(x_share * active, axis=0, keepdims=True),
            ],
            axis=0,
        )
        stage_a[update, me_a, 0:2] = sums
        send_group(
            1,
            4 * update + 1,
            lambda other: stage_a.at[update, me_a, 0:2],
            stage_a.at[update, me_a, 0:2],
        )
        if not last:
            gathered_q[load] = q_share
            send_group(0, 3, lambda other: gathered_q.at[load], gathered_q.at[load])
            await_group(group_recv, 3, gathered_q.at[0 : loads - 1])
            for part in range(loads):
                for plane in range(planes):
                    q_buf[BELOW + plane, 2 * part : 2 * part + 2] = gathered_q[
                        part, 2 * plane : 2 * plane + 2
                    ]
            q_halo = halo(q_buf, (), BELOW, BELOW, 0, q_halo_send, q_halo_recv)
        await_group(group_recv, 4 * update + 1, stage_a.at[update, 0:15, 0:2])
        stage_b[update, me_b, 0:2] = jnp.sum(stage_a[update, :, 0:2], axis=0)
        send_group(
            2,
            4 * update + 2,
            lambda other: stage_b.at[update, me_b, 0:2],
            stage_b.at[update, me_b, 0:2],
        )
        if not last:
            for copy in u_halos[1] + q_halo:
                copy.wait_recv()

    scale = inverse_scale(1)
    lower = jnp.maximum(density_floor, x_share - move_limit)
    upper = jnp.minimum(1.0, x_share + move_limit)
    density_out[...] = jnp.minimum(jnp.maximum(q_share * scale, lower), upper)
    writes.wait()
    for copies_out in (*u_halos, f_halo, x_halo, q_halo):
        for copy in copies_out:
            copy.wait_send()
    for update in range(UPDATES):
        await_group(group_send, 4 * update, gathered_energy.at[update, 0 : loads - 1])
        await_group(group_send, 4 * update + 1, stage_a.at[update, 0:15, 0:2])
        await_group(group_send, 4 * update + 2, stage_b.at[update, 0:31, 0:2])
    await_group(group_send, 3, gathered_q.at[0 : loads - 1])


def body(slabs, loads, density, passive, fixed, u_start, load_nodes, load_forces):
    stiff = element_stiffness()
    center, half_width, ratio_sigma = cheb_constants(stiff)
    weights = cheb_weights(SWEEPS, half_width, ratio_sigma)
    planes, rows, cols = density.shape
    wide = BELOW + planes + ABOVE
    tall = rows + 8
    f32, i32 = jnp.float32, jnp.int32
    vmem = pltpu.VMEM
    dma = pltpu.SemaphoreType.DMA
    hbm = pl.BlockSpec(memory_space=pl.ANY)
    local = pl.BlockSpec(memory_space=pltpu.VMEM)
    new_density, displacement = pl.pallas_call(
        functools.partial(
            kernel,
            mode_constants(stiff),
            (center, weights),
            float(np.mean(diagonal_of(stiff))),
            slabs,
            loads,
        ),
        out_shape=(
            jax.ShapeDtypeStruct((2 * planes, cols), f32),
            jax.ShapeDtypeStruct((3, planes, rows, cols), f32),
        ),
        in_specs=[hbm, hbm, hbm, hbm, local, local],
        out_specs=(local, hbm),
        scratch_shapes=[
            vmem((wide, rows, cols), i32),
            vmem((2, wide - 1, rows, cols), f32),
            vmem((planes, rows, cols), i32),
            vmem((2, 3, wide, rows, cols), f32),
            vmem((2, 3, wide, tall, cols), f32),
            vmem((3, wide - 2, tall, cols), f32),
            vmem((3, wide - 4, tall, cols), f32),
            vmem((3, wide - 6, tall, cols), f32),
            vmem((3, wide - 2, rows, cols), f32),
            vmem((2, wide - 1, rows, cols), f32),
            vmem((wide - 2, rows, cols), f32),
            vmem((3, wide - 2, rows, cols), f32),
            vmem((loads, 8, cols), f32),
            vmem((loads, 8, cols), f32),
            vmem((2, loads, 8, cols), f32),
            vmem((2, loads, 8, cols), f32),
            vmem((loads, 8, cols), f32),
            vmem((wide - 1, rows, cols), f32),
            vmem((2, 16, 8, cols), f32),
            vmem((2, 32, 8, cols), f32),
            dma((4,)),
            dma((8,)),
            dma((8,)),
            dma((2,)),
            dma((2,)),
            dma((8,)),
            dma((8,)),
        ],
        compiler_params=pltpu.CompilerParams(collective_id=0, has_side_effects=True),
        name="updates",
    )(density, passive, fixed, u_start[0], load_nodes, load_forces)
    return new_density.reshape(planes, 2, cols), displacement[None]


def solution(mesh):
    placed = (
        P("slab", None, None),
        P("slab", None, None),
        P("slab", None, None),
        P("load", None, "slab", None, None),
        P("load", None),
        P("load", None, None),
    )
    return jax.shard_map(
        functools.partial(body, mesh.shape["slab"], mesh.shape["load"]),
        mesh=mesh,
        in_specs=placed,
        out_specs=(P("slab", "load", None), P("load", None, "slab", None, None)),
        check_vma=False,
    )
```

```python
import functools
import math

import jax
import jax.numpy as jnp
import numpy as np
from jax import lax
from jax.experimental import pallas as pl
from jax.experimental.pallas import tpu as pltpu
from jax.sharding import PartitionSpec as P

SWEEPS = 3
UPDATES = 2
MESH = pl.DeviceIdType.MESH
young_floor = 0.001
density_floor = 0.001
move_limit = 0.2
sens_shift = 0.001
BELOW = 3
ABOVE = 4


def diagonal_of(matrix):
    return np.array([matrix[entry, entry] for entry in range(matrix.shape[0])])


def element_stiffness():
    poisson = 0.3
    lame_first = poisson / ((1.0 + poisson) * (1.0 - 2.0 * poisson))
    lame_second = 1.0 / (2.0 * (1.0 + poisson))
    elastic = np.zeros((6, 6))
    elastic[:3, :3] = lame_first
    for axis_pos in range(3):
        elastic[axis_pos, axis_pos] += 2.0 * lame_second
        elastic[axis_pos + 3, axis_pos + 3] = lame_second
    points = [0.5 - 0.5 / math.sqrt(3.0), 0.5 + 0.5 / math.sqrt(3.0)]
    matrix = np.zeros((24, 24))
    for point_x in points:
        for point_y in points:
            for point_z in points:
                strain = np.zeros((6, 24))
                for corner in range(8):
                    shift_x = corner % 2
                    shift_y = corner // 2 % 2
                    shift_z = corner // 4
                    value_x = point_x if shift_x else 1.0 - point_x
                    value_y = point_y if shift_y else 1.0 - point_y
                    value_z = point_z if shift_z else 1.0 - point_z
                    slope_x = 1.0 if shift_x else -1.0
                    slope_y = 1.0 if shift_y else -1.0
                    slope_z = 1.0 if shift_z else -1.0
                    grad_x = slope_x * value_y * value_z
                    grad_y = value_x * slope_y * value_z
                    grad_z = value_x * value_y * slope_z
                    column = 3 * corner
                    strain[0, column] = grad_x
                    strain[1, column + 1] = grad_y
                    strain[2, column + 2] = grad_z
                    strain[3, column] = grad_y
                    strain[3, column + 1] = grad_x
                    strain[4, column + 1] = grad_z
                    strain[4, column + 2] = grad_y
                    strain[5, column] = grad_z
                    strain[5, column + 2] = grad_x
                matrix += strain.T @ elastic @ strain / 8.0
    return matrix


def spectrum_top(matrix):
    diag_np = diagonal_of(matrix)
    scaled = matrix / np.sqrt(np.outer(diag_np, diag_np))
    vector = np.linspace(1.0, 2.0, 24)
    for repeat in range(500):
        vector = scaled @ vector
        vector = vector / np.sqrt(np.sum(vector * vector))
    return float(vector @ scaled @ vector)


def cheb_constants(matrix):
    upper_bound = 1.05 * spectrum_top(matrix)
    lower_bound = upper_bound / 12.0
    center = 0.5 * (upper_bound + lower_bound)
    half_width = 0.5 * (upper_bound - lower_bound)
    return (center, half_width, center / half_width)


def cheb_weights(count, half_width, ratio_sigma):
    weights = []
    current = 1.0 / ratio_sigma
    for iteration in range(count):
        following = 1.0 / (2.0 * ratio_sigma - current)
        weights.append((following * current, 2.0 * following / half_width))
        current = following
    return weights


def parity_stiffness(matrix):
    transform = np.zeros((24, 24))
    for mode in range(8):
        for corner in range(8):
            sign = 1.0
            for axis in range(3):
                if (mode >> axis) & 1 and not (corner >> axis) & 1:
                    sign = -sign
            for part in range(3):
                transform[3 * mode + part, 3 * corner + part] = sign
    return transform @ matrix @ transform.T / 64.0


def mode_constants(matrix):
    block = parity_stiffness(matrix)

    def entry(part_a, mode_a, part_b, mode_b):
        def index(part, mode):
            return 3 * sum(1 << axis for axis in range(3) if mode[axis] == "d") + part

        return float(block[index(part_a, mode_a), index(part_b, mode_b)])

    cross = entry(0, "dss", 1, "sds")
    return dict(
        cross=cross,
        normal=entry(0, "dss", 0, "dss") - cross,
        shear=entry(0, "sds", 1, "dss"),
        bend=entry(0, "dds", 0, "dds"),
        couple=entry(0, "dds", 2, "sdd"),
        twist=entry(0, "sdd", 1, "dsd"),
        warp=entry(0, "ddd", 0, "ddd"),
    )


def right_of(value, lane):
    return jnp.where(lane == value.shape[1] - 1, 0.0, pltpu.roll(value, value.shape[1] - 1, 1))


def left_of(value, lane):
    return jnp.where(lane == 0, 0.0, pltpu.roll(value, 1, 1))


def under_of(value, row):
    return jnp.where(row == 0, 0.0, pltpu.roll(value, 1, 0))


def plane_modes(ref, plane, start, lane):
    rows = lane.shape[0]
    found = []
    for part in range(3):
        near = ref[part, plane, start : start + rows, :]
        far = ref[part, plane, start + 1 : start + 1 + rows, :]
        for value in (near + far, far - near):
            other = right_of(value, lane)
            found += [value + other, other - value]
    return found


def element_modes(low, high):
    names = ("ss", "ds", "sd", "dd")
    modes = {}
    for part in range(3):
        for place, name in enumerate(names):
            low_value, high_value = low[4 * part + place], high[4 * part + place]
            if name != "ss":
                modes["xyz"[part] + name + "s"] = low_value + high_value
            modes["xyz"[part] + name + "d"] = high_value - low_value
    return modes


def stress_modes(m, young, k):
    normal, cross, shear = young * k["normal"], young * k["cross"], young * k["shear"]
    bend, couple, twist = young * k["bend"], young * k["couple"], young * k["twist"]
    warp = young * k["warp"]
    out = {}
    trace = cross * (m["xdss"] + m["ysds"] + m["zssd"])
    for name in ("xdss", "ysds", "zssd"):
        out[name] = normal * m[name] + trace
    for first, second in (("ydss", "xsds"), ("zdss", "xssd"), ("zsds", "yssd")):
        out[first] = out[second] = shear * (m[first] + m[second])
    for first, second in (("xdds", "zsdd"), ("ydds", "zdsd"), ("xdsd", "ysdd")):
        out[first] = bend * m[first] + couple * m[second]
        out[second] = couple * m[first] + bend * m[second]
    total = m["zdds"] + m["ydsd"] + m["xsdd"]
    for name in ("zdds", "ydsd", "xsdd"):
        out[name] = twist * (m[name] + total)
    for name in ("xddd", "yddd", "zddd"):
        out[name] = warp * m[name]
    return out


def energy_of(m, k):
    def squares(names):
        return sum((m[name] * m[name] for name in names[1:]), m[names[0]] * m[names[0]])

    normals = ("xdss", "ysds", "zssd")
    twists = ("zdds", "ydsd", "xsdd")
    trace = m["xdss"] + m["ysds"] + m["zssd"]
    result = k["normal"] * squares(normals) + k["cross"] * (trace * trace)
    shears = None
    for first, second in (("ydss", "xsds"), ("zdss", "xssd"), ("zsds", "yssd")):
        value = m[first] + m[second]
        shears = value * value if shears is None else shears + value * value
    result = result + k["shear"] * shears
    pairs = (("xdds", "zsdd"), ("ydds", "zdsd"), ("xdsd", "ysdd"))
    result = result + k["bend"] * squares([name for pair in pairs for name in pair])
    products = sum(
        (m[first] * m[second] for first, second in pairs[1:]), m[pairs[0][0]] * m[pairs[0][1]]
    )
    result = result + (2.0 * k["couple"]) * products
    total = m["zdds"] + m["ydsd"] + m["xsdd"]
    result = result + k["twist"] * (squares(twists) + total * total)
    return result + k["warp"] * squares(("xddd", "yddd", "zddd"))


def node_parts(out):
    lower, upper = [], []
    for part in "xyz":
        for name in ("ss", "ds", "sd", "dd"):
            odd = out[part + name + "d"]
            if name == "ss":
                lower.append(-odd)
                upper.append(odd)
            else:
                even = out[part + name + "s"]
                lower.append(even - odd)
                upper.append(even + odd)
    return lower, upper


def node_rows(sums, lane):
    rows = []
    for part in range(3):
        both, along, across, twice = sums[4 * part : 4 * part + 4]
        even = (both - along) + left_of(both + along, lane)
        odd = (across - twice) + left_of(across + twice, lane)
        rows.append((even - odd, even + odd))
    return rows


def apply_stiffness(ref, first, count, young_ref, young_first, k, lane, row, seam, emit):
    half = lane.shape[0]
    for part_of_plane in range(2):
        start = part_of_plane * half
        rows = slice(start, start + half)
        low = plane_modes(ref, first - 1, start, lane)
        high = plane_modes(ref, first, start, lane)
        out = stress_modes(element_modes(low, high), young_ref[young_first - 1, rows], k)
        pending = node_parts(out)[1]

        def step(turn, carry):
            low, pending = carry
            high = plane_modes(ref, first + 1 + turn, start, lane)
            out = stress_modes(element_modes(low, high), young_ref[young_first + turn, rows], k)
            lower, upper = node_parts(out)
            forces = []
            pairs = node_rows([a + b for a, b in zip(lower, pending)], lane)
            for part, (near, far) in enumerate(pairs):
                turned = pltpu.roll(far, 1, 0)
                if start == 0:
                    seam[part, turn] = turned
                    above = 0.0
                else:
                    above = seam[part, turn]
                forces.append(near + jnp.where(row == 0, above, turned))
            emit(turn, rows, forces)
            return high, upper

        lax.fori_loop(0, count, step, (high, pending), unroll=True)


def kernel(
    k, chebyshev, stiff_diag, slabs, loads,
    density_hbm, passive_hbm, fixed_hbm, start_hbm, nodes_hbm, points_hbm,
    density_out, displace_out,
    nodes_ref, points_ref, fixed_buf, design_buf, passive_buf, raw_buf, masked_buf, first_dir, second_dir, final_buf,
    residual, seam, young_buf, weight_buf, force_buf, share_design, share_active, share_energy,
    gathered_energy, gathered_q, q_buf, stage_a, stage_b, local_sem, halo_send, halo_recv,
    q_halo_send, q_halo_recv, group_send, group_recv,
):
    center, weights = chebyshev
    slab = lax.axis_index("slab")
    load = lax.axis_index("load")
    planes, rows, cols = passive_buf.shape
    own = slice(BELOW, BELOW + planes)
    lane = lax.broadcasted_iota(jnp.int32, (rows, cols), 1)
    row = lax.broadcasted_iota(jnp.int32, (rows, cols), 0)
    half_lane = lax.broadcasted_iota(jnp.int32, (rows // 2, cols), 1)
    half_row = lax.broadcasted_iota(jnp.int32, (rows // 2, cols), 0)
    up = lax.rem(slab + 1, slabs)
    down = lax.rem(slab + slabs - 1, slabs)
    column = lax.div(slab, 8)
    seat = lax.rem(slab, 8)
    x_place = lax.div(load, 2)
    y_low = lax.rem(load, 2)
    y_place = lax.div(seat, 2) * 2 + y_low
    core = lax.rem(seat, 2)
    me_a = y_place * 2 + core
    me_b = column * 4 + x_place
    slab_at = [lax.rem(column + step, 8) * 8 + seat for step in range(8)]
    load_at = [lax.rem(x_place + step, 4) * 2 for step in range(4)]
    y_at = [lax.rem(y_place + step, 8) for step in range(8)]
    y_slab = [column * 8 + lax.div(y, 2) * 2 for y in y_at]
    y_load = [load - y_low + lax.rem(y, 2) for y in y_at]
    cores = (core, 1 - core)
    lows = (y_low, 1 - y_low)

    def near(step, size):
        return min(step, size - step)

    def by_distance(pairs, size, other):
        order = sorted(pairs, key=lambda p: -(near(p[0], size) + near(p[1], other)))
        return [p for p in order if p != (0, 0)]

    over_load = [
        (load_at[step] + lows[low], (slab, load_at[step] + lows[low]))
        for step, low in by_distance([(i, j) for i in range(4) for j in range(2)], 4, 2)
    ]
    over_a = [
        (None, (y_slab[step] + cores[flip], y_load[step]))
        for step, flip in by_distance([(i, j) for i in range(8) for j in range(2)], 8, 2)
    ]
    over_b = [
        (None, (slab_at[up_by], load_at[step] + y_low))
        for up_by, step in by_distance([(i, j) for i in range(8) for j in range(4)], 8, 4)
    ]
    groups = (over_load, over_a, over_b)

    copies = [
        pltpu.make_async_copy(start_hbm, raw_buf.at[0, :, own], local_sem.at[0]),
        pltpu.make_async_copy(fixed_hbm, fixed_buf.at[own], local_sem.at[1]),
        pltpu.make_async_copy(density_hbm, design_buf.at[0, own], local_sem.at[2]),
        pltpu.make_async_copy(passive_hbm, passive_buf, local_sem.at[3]),
        pltpu.make_async_copy(nodes_hbm, nodes_ref, local_sem.at[4]),
        pltpu.make_async_copy(points_hbm, points_ref, local_sem.at[5]),
    ]
    for copy in copies:
        copy.start()

    barrier = pltpu.get_barrier_semaphore()
    for target in ((up, load), (down, load)):
        pl.semaphore_signal(barrier, inc=1, device_id=target, device_id_type=MESH)
    for group in groups:
        for _, who in group:
            pl.semaphore_signal(barrier, inc=1, device_id=who, device_id_type=MESH)

    for copy in copies:
        copy.wait()
    for plane in range(planes):
        void = passive_buf[plane] == 1
        value = jnp.where(void, density_floor, design_buf[0, BELOW + plane])
        design_buf[0, BELOW + plane] = value
        active = 1.0 - passive_buf[plane].astype(jnp.float32)
        for part in range(loads):
            share_design[part, 2 * plane : 2 * plane + 2] = value[2 * part : 2 * part + 2]
            share_active[part, 2 * plane : 2 * plane + 2] = active[2 * part : 2 * part + 2]
    pl.semaphore_wait(barrier, 2 + sum(len(group) for group in groups))

    def halo(buf, lead, upward, downward, index, send, recv):
        top = BELOW + planes
        pairs = (
            (slice(top - upward, top), slice(BELOW - upward, BELOW), up),
            (slice(BELOW, BELOW + downward), slice(top, top + downward), down),
        )
        made = []
        for place, (source, target, who) in enumerate(pairs):
            made.append(
                pltpu.make_async_remote_copy(
                    buf.at[lead + (source,)],
                    buf.at[lead + (target,)],
                    send.at[2 * index + place],
                    recv.at[2 * index + place],
                    device_id=(who, load),
                    device_id_type=MESH,
                )
            )
        for copy in made:
            copy.start()
        return made

    def send_group(group, index, source, target):
        for other, who in groups[group]:
            pltpu.make_async_remote_copy(
                source(other),
                target,
                group_send.at[index],
                group_recv.at[index],
                device_id=who,
                device_id_type=MESH,
            ).start()

    def await_group(sem, index, ref):
        pltpu.make_async_copy(ref, ref, sem.at[index]).wait()

    x_halo = halo(design_buf, (0,), BELOW, BELOW, 2, halo_send, halo_recv)
    f_halo = halo(fixed_buf, (), BELOW, ABOVE, 1, halo_send, halo_recv)
    u_halos = [halo(raw_buf, (0, slice(None)), BELOW, ABOVE, 0, halo_send, halo_recv)]

    edge = jnp.zeros((8, cols), jnp.float32)
    for part in range(3):
        for buf in (first_dir, second_dir, final_buf):
            for plane in range(buf.shape[1]):
                buf[part, plane, rows : rows + 8] = edge
        for plane in range(masked_buf.shape[2]):
            masked_buf[0, part, plane, rows : rows + 8] = edge
            masked_buf[1, part, plane, rows : rows + 8] = edge

    nodes = nodes_ref[...]
    points = nodes.shape[1]
    tall = 9 * rows
    place_zy = lax.broadcasted_iota(jnp.int32, (tall, points), 0) + (slab * planes - 2) * rows
    hit_zy = jnp.where(lax.div(nodes, cols) == place_zy, 1.0, 0.0)
    hit_x = lax.rem(nodes, cols) == lax.broadcasted_iota(jnp.int32, (cols, points), 0)
    for part in range(3):
        amount = jnp.where(hit_x, points_ref[part], 0.0)
        force_buf[part] = lax.dot_general(
            hit_zy,
            amount,
            (((1,), (1,)), ((), ())),
            precision=lax.Precision.HIGHEST,
            preferred_element_type=jnp.float32,
        ).reshape(9, rows, cols)

    has_below = jnp.where(slab > 0, 1.0, 0.0)
    has_above = jnp.where(slab < slabs - 1, 1.0, 0.0)

    def young_planes(which):
        for plane in range(10):
            x = design_buf[which, plane]
            young = young_floor + (1.0 - young_floor) * x * x * x
            if plane < BELOW:
                young = young * has_below
            elif plane >= BELOW + planes:
                young = young * has_above
            young_buf[which, plane] = young

    def weights_of(update):
        for node in range(9):
            free = 1.0 - fixed_buf[node + 1].astype(jnp.float32)
            if node < 2:
                free = free * has_below
            elif node >= 2 + planes:
                free = free * has_above
            around = young_buf[update, node] + young_buf[update, node + 1]
            around = around + under_of(around, row)
            around = around + left_of(around, lane)
            weight_buf[node] = free / jnp.maximum(stiff_diag * around, 1e-6)

    for copy in x_halo + f_halo:
        copy.wait_recv()
    young_planes(0)
    weights_of(0)
    for copy in u_halos[0]:
        copy.wait_recv()

    def inverse_scale(update):
        await_group(group_recv, 4 * update + 2, stage_b.at[update, 0:31, 0:2])
        sums = jnp.sum(jnp.sum(stage_b[update, :, 0:2], axis=0), axis=1, keepdims=True)
        top, bottom = sums[0:1], sums[1:2]
        ratio = bottom / jnp.where(top > 0.0, top, 1.0)
        return jnp.where(top > 0.0, ratio, 0.0)

    for update in range(UPDATES):
        last = update == UPDATES - 1
        for plane in range(11):
            free = 1.0 - fixed_buf[plane].astype(jnp.float32)
            if plane < BELOW:
                free = free * has_below
            elif plane >= BELOW + planes:
                free = free * has_above
            for part in range(3):
                masked_buf[update, part, plane, 0:rows] = free * raw_buf[update, part, plane]
        if update:
            scale = inverse_scale(0)
            for plane in range(10):
                x = design_buf[0, plane]
                lower = jnp.maximum(density_floor, x - move_limit)
                upper = jnp.minimum(1.0, x + move_limit)
                design_buf[1, plane] = jnp.minimum(
                    jnp.maximum(q_buf[plane] * scale, lower), upper
                )
            young_planes(1)
            weights_of(1)

        field = masked_buf.at[update]
        young = young_buf.at[update]

        def start_stage(turn, part_rows, forces):
            weight = weight_buf[turn, part_rows]
            for part in range(3):
                left = force_buf[part, turn, part_rows] - forces[part]
                residual[part, turn, part_rows] = left
                first_dir[part, turn, part_rows] = (weight * (1.0 / center)) * left

        apply_stiffness(
            field, 1, 9, young, 1, k, half_lane, half_row, seam, start_stage
        )

        def middle_stage(turn, part_rows, forces):
            keep, push = weights[0]
            weight = push * weight_buf[turn + 1, part_rows]
            for part in range(3):
                left = residual[part, turn + 1, part_rows] - forces[part]
                residual[part, turn + 1, part_rows] = left
                second_dir[part, turn, part_rows] = (
                    keep * first_dir[part, turn + 1, part_rows] + weight * left
                )

        apply_stiffness(
            first_dir, 1, 7, young, 2, k, half_lane, half_row, seam, middle_stage
        )

        def final_stage(turn, part_rows, forces):
            keep, push = weights[1]
            weight = push * weight_buf[turn + 2, part_rows]
            for part in range(3):
                left = residual[part, turn + 2, part_rows] - forces[part]
                final_buf[part, turn, part_rows] = (
                    field[part, turn + BELOW, part_rows]
                    + first_dir[part, turn + 2, part_rows]
                    + (1.0 + keep) * second_dir[part, turn + 1, part_rows]
                    + weight * left
                )

        apply_stiffness(
            second_dir, 1, 5, young, 3, k, half_lane, half_row, seam, final_stage
        )

        if not last:
            for part in range(3):
                raw_buf[1, part, own] = final_buf[part, 0:planes, 0:rows]
            u_halos.append(halo(raw_buf, (1, slice(None)), BELOW, ABOVE, 3, halo_send, halo_recv))
        else:
            displace_out[...] = final_buf[:, 0:planes, 0:rows]

        for start in (0, rows // 2):
            low = plane_modes(final_buf, 0, start, half_lane)
            for plane in range(planes):
                high = plane_modes(final_buf, plane + 1, start, half_lane)
                energy = energy_of(element_modes(low, high), k)
                for pair in range(rows // 4):
                    share_energy[update, start // 2 + pair, 2 * plane : 2 * plane + 2] = energy[
                        2 * pair : 2 * pair + 2
                    ]
                low = high
        gathered_energy[update, load] = share_energy[update, load]
        send_group(
            0, 4 * update, lambda other: share_energy.at[update, other], gathered_energy.at[update, load]
        )

        if update == 0:
            x_share = share_design[load]
        else:
            lower = jnp.maximum(density_floor, x_share - move_limit)
            upper = jnp.minimum(1.0, x_share + move_limit)
            x_share = jnp.minimum(jnp.maximum(q_share * scale, lower), upper)
        active = share_active[load]
        await_group(group_recv, 4 * update, gathered_energy.at[update, 0 : loads - 1])
        total = gathered_energy[update, 0]
        for part in range(1, loads):
            total = total + gathered_energy[update, part]
        q_share = (
            x_share
            * jnp.sqrt(3.0 * x_share * x_share * (1.0 - young_floor) * total + sens_shift)
            * active
        )
        sums = jnp.concatenate(
            [
                jnp.sum(q_share, axis=0, keepdims=True),
                jnp.sum(x_share * active, axis=0, keepdims=True),
            ],
            axis=0,
        )
        stage_a[update, me_a, 0:2] = sums
        send_group(
            1,
            4 * update + 1,
            lambda other: stage_a.at[update, me_a, 0:2],
            stage_a.at[update, me_a, 0:2],
        )
        if not last:
            gathered_q[load] = q_share
            send_group(0, 3, lambda other: gathered_q.at[load], gathered_q.at[load])
        await_group(group_recv, 4 * update + 1, stage_a.at[update, 0:15, 0:2])
        stage_b[update, me_b, 0:2] = jnp.sum(stage_a[update, :, 0:2], axis=0)
        send_group(
            2,
            4 * update + 2,
            lambda other: stage_b.at[update, me_b, 0:2],
            stage_b.at[update, me_b, 0:2],
        )
        if not last:
            await_group(group_recv, 3, gathered_q.at[0 : loads - 1])
            for part in range(loads):
                for plane in range(planes):
                    q_buf[BELOW + plane, 2 * part : 2 * part + 2] = gathered_q[
                        part, 2 * plane : 2 * plane + 2
                    ]
            q_halo = halo(q_buf, (), BELOW, BELOW, 0, q_halo_send, q_halo_recv)
            for copy in u_halos[1] + q_halo:
                copy.wait_recv()

    scale = inverse_scale(1)
    lower = jnp.maximum(density_floor, x_share - move_limit)
    upper = jnp.minimum(1.0, x_share + move_limit)
    density_out[...] = jnp.minimum(jnp.maximum(q_share * scale, lower), upper)
    for copies_out in (*u_halos, f_halo, x_halo, q_halo):
        for copy in copies_out:
            copy.wait_send()
    for update in range(UPDATES):
        await_group(group_send, 4 * update, gathered_energy.at[update, 0 : loads - 1])
        await_group(group_send, 4 * update + 1, stage_a.at[update, 0:15, 0:2])
        await_group(group_send, 4 * update + 2, stage_b.at[update, 0:31, 0:2])
    await_group(group_send, 3, gathered_q.at[0 : loads - 1])


def deliver(share, displacement):
    parts, planes, rows, cols = displacement.shape

    def kernel(share_ref, source_ref, density_out, displace_out, split, sems):
        first = pltpu.make_async_copy(source_ref, displace_out.at[0], sems.at[0])
        first.start()
        for plane in range(planes):
            split[plane] = share_ref[2 * plane : 2 * plane + 2]
        second = pltpu.make_async_copy(split, density_out, sems.at[1])
        second.start()
        second.wait()
        first.wait()

    hbm = pl.BlockSpec(memory_space=pl.ANY)
    local = pl.BlockSpec(memory_space=pltpu.VMEM)
    return pl.pallas_call(
        kernel,
        out_shape=(
            jax.ShapeDtypeStruct((planes, 2, cols), jnp.float32),
            jax.ShapeDtypeStruct((1, parts, planes, rows, cols), jnp.float32),
        ),
        in_specs=[local, local],
        out_specs=(hbm, hbm),
        scratch_shapes=[
            pltpu.VMEM((planes, 2, cols), jnp.float32),
            pltpu.SemaphoreType.DMA((2,)),
        ],
        name="deliver",
    )(
        pltpu.with_memory_space_constraint(share, pltpu.VMEM),
        pltpu.with_memory_space_constraint(displacement, pltpu.VMEM),
    )


def body(slabs, loads, density, passive, fixed, u_start, load_nodes, load_forces):
    stiff = element_stiffness()
    center, half_width, ratio_sigma = cheb_constants(stiff)
    weights = cheb_weights(SWEEPS, half_width, ratio_sigma)
    planes, rows, cols = density.shape
    wide = BELOW + planes + ABOVE
    tall = rows + 8
    f32, i32 = jnp.float32, jnp.int32
    vmem = pltpu.VMEM
    dma = pltpu.SemaphoreType.DMA
    hbm = pl.BlockSpec(memory_space=pl.ANY)
    local = pl.BlockSpec(memory_space=pltpu.VMEM)
    new_density, displacement = pl.pallas_call(
        functools.partial(
            kernel,
            mode_constants(stiff),
            (center, weights),
            float(np.mean(diagonal_of(stiff))),
            slabs,
            loads,
        ),
        out_shape=(
            pltpu.VMEM((2 * planes, cols), f32),
            pltpu.VMEM((3, planes, rows, cols), f32),
        ),
        in_specs=[hbm] * 6,
        out_specs=(local, local),
        scratch_shapes=[
            vmem(load_nodes.shape, i32),
            vmem((3, 1, load_nodes.shape[1]), f32),
            vmem((wide, rows, cols), i32),
            vmem((2, wide - 1, rows, cols), f32),
            vmem((planes, rows, cols), i32),
            vmem((2, 3, wide, rows, cols), f32),
            vmem((2, 3, wide, tall, cols), f32),
            vmem((3, wide - 2, tall, cols), f32),
            vmem((3, wide - 4, tall, cols), f32),
            vmem((3, wide - 6, tall, cols), f32),
            vmem((3, wide - 2, rows, cols), f32),
            vmem((3, wide - 2, rows // 2, cols), f32),
            vmem((2, wide - 1, rows, cols), f32),
            vmem((wide - 2, rows, cols), f32),
            vmem((3, wide - 2, rows, cols), f32),
            vmem((loads, 8, cols), f32),
            vmem((loads, 8, cols), f32),
            vmem((2, loads, 8, cols), f32),
            vmem((2, loads, 8, cols), f32),
            vmem((loads, 8, cols), f32),
            vmem((wide - 1, rows, cols), f32),
            vmem((2, 16, 8, cols), f32),
            vmem((2, 32, 8, cols), f32),
            dma((6,)),
            dma((8,)),
            dma((8,)),
            dma((2,)),
            dma((2,)),
            dma((8,)),
            dma((8,)),
        ],
        compiler_params=pltpu.CompilerParams(collective_id=0, has_side_effects=True),
        name="updates",
    )(density, passive, fixed, u_start[0], load_nodes, load_forces.transpose(1, 0, 2))
    return deliver(new_density, displacement)


def solution(mesh):
    placed = (
        P("slab", None, None),
        P("slab", None, None),
        P("slab", None, None),
        P("load", None, "slab", None, None),
        P("load", None),
        P("load", None, None),
    )
    return jax.shard_map(
        functools.partial(body, mesh.shape["slab"], mesh.shape["load"]),
        mesh=mesh,
        in_specs=placed,
        out_specs=(P("slab", "load", None), P("load", None, "slab", None, None)),
        check_vma=False,
    )
```
